32 devices in a mesh: gx: 4 (over y, x), gy: 4 (over z), gz: 2 (over core).
Axes of the slice: x: 2, y: 2, z: 4, core: 2. Of those that a mesh axis runs over, the one named last changes fastest.
Arguments:
- right_side: float32 [64, 256, 1024], P('gx', 'gy', 'gz'), may hold values from -24 to 24
- reaction: float32 [64, 256, 1024], P('gx', 'gy', 'gz'), may hold values from 0.5 to 2
- velocity: float32 [3, 64, 256, 1024], P(None, 'gx', 'gy', 'gz'), may hold values from -0.5 to 0.5
Outputs:
- solution: float32 [64, 256, 1024], P('gx', 'gy', 'gz')
- residual: float32 [64, 256, 1024], P('gx', 'gy', 'gz')
- residual_norm: float32 [], replicated
The draws below stay inside these ranges and needn't reach their ends.
All inputs are finite; a program needn't handle non-finite values.
Results may differ from the reference program's by a relative error of at most 0.00002.
Values sent between devices are 32-bit elements; how exact they have to be, the bound alone decides.
A program may use at most 128 MiB of HBM per device.

```python
import math
import jax
import jax.numpy as jnp

ITERS = 5
NX = 64
NY = 256
NZ = 1024


def draw_right_side(key, part):
    noise_key = jax.random.fold_in(jax.random.fold_in(key, 11), 0)
    ramp = 1.0 + 2.0 * jnp.arange(NX, dtype=jnp.float32)[:, None, None] / max(NX - 1, 1)
    values = ramp * jnp.clip(jax.random.normal(noise_key, (NX, NY, NZ), jnp.float32), -6.0, 6.0)
    return values.astype(jnp.float32)


def block_levels(own_key, extent, shards, least, top_value):
    def one(position, blocks):
        steps = jax.random.uniform(jax.random.fold_in(jax.random.fold_in(own_key, 6), position), (blocks,), jnp.float32, least / len(shards), top_value / len(shards))
        return jnp.repeat(jnp.exp(steps), extent[position] // blocks).reshape((-1,) + (1,) * (len(extent) - position - 1))

    loudness = one(*shards[0])
    for cut in shards[1:]:
        loudness = loudness * one(*cut)
    return loudness


def setup_inputs(seed: int = 0) -> dict:
    arg_keys = jax.random.split(jax.random.key(seed), 4)
    return {
        "right_side": draw_right_side(jax.random.fold_in(arg_keys[3], 71), 0),
        "reaction": jnp.clip(jnp.exp(math.log(2.0) - 1.3862944 * jax.random.uniform(arg_keys[1], (NX, NY, NZ), jnp.float32) ** block_levels(arg_keys[1], (NX, NY, NZ), ((0, 4), (1, 4), (2, 2)), -0.2, 0.2)), 0.5, 2.0),
        "velocity": jnp.clip(jax.random.uniform(arg_keys[2], (3, NX, NY, NZ), jnp.float32, -0.5, 0.5) * block_levels(arg_keys[2], (3, NX, NY, NZ), ((1, 4), (2, 4), (3, 2)), -0.4, 0.0), -0.5, 0.5),
    }


centre = 7.25
half_width = 6.75

def chebyshev_weights(count):
    ratio_value = centre / half_width
    weights = [1.0 / ratio_value]
    for iteration in range(count):
        weights.append(1.0 / (2.0 * ratio_value - weights[-1]))
    return weights

def combine(middle, plus_x, minus_x, plus_y, minus_y, plus_z, minus_z, reaction, velocity):
    beside = (1.0 - velocity[0]) * plus_x + (1.0 + velocity[0]) * minus_x
    beside = beside + (1.0 - velocity[1]) * plus_y + (1.0 + velocity[1]) * minus_y
    beside = beside + (1.0 - velocity[2]) * plus_z + (1.0 + velocity[2]) * minus_z
    return (6.0 + reaction) * middle - beside

def operate(values, reaction, velocity):
    plus_x = jnp.roll(values, -1, 0)
    minus_x = jnp.roll(values, 1, 0)
    padded = jnp.pad(values, ((0, 0), (1, 1), (1, 1)))
    return combine(values, plus_x, minus_x, padded[:, 2:, 1:-1], padded[:, :-2, 1:-1], padded[:, 1:-1, 2:], padded[:, 1:-1, :-2], reaction, velocity)

def reference(right_side, reaction, velocity):
    weights = chebyshev_weights(ITERS)
    solution = jnp.zeros_like(right_side)
    residual = right_side
    direction = right_side / centre
    for iteration in range(ITERS):
        applied = operate(direction, reaction, velocity)
        solution = solution + direction
        residual = residual - applied
        if iteration + 1 < ITERS:
            direction = weights[iteration + 1] * weights[iteration] * direction + 2.0 * weights[iteration + 1] / half_width * residual
    residual_norm = jnp.sqrt(jnp.sum(residual * residual) / (NX * NY * NZ) + 1e-06)
    return (solution, residual, residual_norm)
```

```python
import functools
import itertools

import jax
import jax.numpy as jnp
from jax import lax
from jax.experimental import pallas as pl
from jax.experimental.pallas import tpu as pltpu
from jax.sharding import PartitionSpec as P

ITERS = 5
CHUNKS = 4
ROWS = 8
GROUP = 7

centre = 7.25
half_width = 6.75

AXES = ("gx", "gy", "gz")
PY, PZ = 8, 128
LOW, HIGH = 0, 1


def chebyshev_weights(count):
    ratio_value = centre / half_width
    weights = [1.0 / ratio_value]
    for iteration in range(count):
        weights.append(1.0 / (2.0 * ratio_value - weights[-1]))
    return weights


def reaches(sizes):
    return sizes[0] // 2 + sizes[1] - 1 + sizes[2] - 1 <= ITERS + 1


def phases(sizes):
    return ((0, 1, 2),) if reaches(sizes) else ((2,), (0, 1))


def phase_steps(sizes, axes):
    ranges = [range(n) if i in axes else (0,) for i, n in enumerate(sizes)]
    return [steps for steps in itertools.product(*ranges) if any(steps)]


def greeted_by(sizes):
    steps = {
        tuple(p if j == i else 0 for j in range(len(sizes)))
        for i, n in enumerate(sizes)
        for p in (1, n - 1)
    }
    for axes in phases(sizes):
        steps |= set(phase_steps(sizes, axes))
    return sorted(steps)


def phase_slots(sizes):
    return sum(len(phase_steps(sizes, axes)) + 1 for axes in phases(sizes))


def kernel(
    sizes,
    rhs,
    reaction,
    velocity,
    sol,
    res,
    norm,
    d,
    reac,
    vel,
    ysend,
    yrecv,
    part,
    rhs_sem,
    load_sem,
    xs_sem,
    xr_sem,
    ys_sem,
    yr_sem,
    zs_sem,
    zr_sem,
    ps_sem,
    pr_sem,
):
    nx, ny, nz = rhs.shape
    weights = chebyshev_weights(ITERS)
    me = [lax.axis_index(a) for a in AXES]
    mid_y = pl.ds(PY, ny)
    mid_z = pl.ds(PZ, nz)
    chunk = ny // CHUNKS

    order = [0, CHUNKS - 1] + list(range(1, CHUNKS - 1))
    load_rhs = [
        pltpu.make_async_copy(
            rhs.at[pl.ds(first, count)],
            d.at[0, pl.ds(1 + first, count), mid_y, mid_z],
            rhs_sem.at[i],
        )
        for i, (first, count) in enumerate(((0, 1), (nx - 1, 1), (1, nx - 2)))
    ]
    loads = {}
    for c in order:
        rows = pl.ds(c * chunk, chunk)
        loads[c] = [
            pltpu.make_async_copy(
                reaction.at[:, rows], reac.at[:, rows], load_sem.at[c, 0]
            ),
            pltpu.make_async_copy(
                velocity.at[:, :, rows], vel.at[:, :, rows], load_sem.at[c, 1]
            ),
        ]
    for copy in load_rhs:
        copy.start()
    for c in order:
        for copy in loads[c]:
            copy.start()

    barrier = pltpu.get_barrier_semaphore()
    def shifted(steps):
        return {
            a: lax.rem(i + p, n)
            for a, n, i, p in zip(AXES, sizes, me, steps)
            if p
        }

    def greet(steps):
        pl.semaphore_signal(
            barrier,
            inc=1,
            device_id=shifted(steps),
            device_id_type=pl.DeviceIdType.MESH,
        )

    if reaches(sizes):
        for step in sorted({1, sizes[0] - 1}):
            greet((step, 0, 0))
        greeters = len({1, sizes[0] - 1})
        for axis in (1, 2):
            for step, there in (
                (1, me[axis] < sizes[axis] - 1),
                (sizes[axis] - 1, me[axis] > 0),
            ):
                @pl.when(there)
                def _(axis=axis, step=step):
                    greet(tuple(step if a == axis else 0 for a in range(3)))

                greeters = greeters + there.astype(jnp.int32)
    else:
        for steps in greeted_by(sizes):
            greet(steps)
        greeters = len(greeted_by(sizes))

    for side, at_edge in ((LOW, me[1] == 0), (HIGH, me[1] == sizes[1] - 1)):
        @pl.when(at_edge)
        def _(side=side):
            for slot in range(2):
                yrecv[slot, side] = jnp.zeros((nx, 1, nz), jnp.float32)

    for first, at_edge in ((0, me[2] == 0), (PZ + nz, me[2] == sizes[2] - 1)):
        @pl.when(at_edge)
        def _(first=first):
            def clear(x, carry):
                for slot in range(2):
                    d[slot, x, pl.ds(PY, ny), pl.ds(first, PZ)] = jnp.zeros(
                        (ny, PZ), jnp.float32
                    )
                return carry

            lax.fori_loop(1, nx + 1, clear, 0)

    pl.semaphore_wait(barrier, greeters)

    def remote(src, dst, send, recv, axis, target):
        return pltpu.make_async_remote_copy(
            src_ref=src,
            dst_ref=dst,
            send_sem=send,
            recv_sem=recv,
            device_id={AXES[axis]: target},
            device_id_type=pl.DeviceIdType.MESH,
        )

    def x_copy(slot, side, c):
        n = sizes[0]
        rows = pl.ds(PY + c * chunk, chunk)
        plane, land, target = (
            (nx, 0, lax.rem(me[0] + 1, n))
            if side == LOW
            else (1, nx + 1, lax.rem(me[0] + n - 1, n))
        )
        return remote(
            d.at[slot, plane, rows, mid_z],
            d.at[slot, land, rows, mid_z],
            xs_sem.at[slot, side, c],
            xr_sem.at[slot, side, c],
            0,
            target,
        )

    def target_of(axis, side):
        n = sizes[axis]
        step = 1 if side == LOW else n - 1
        return lax.rem(me[axis] + step, n)

    def sends(axis, side):
        return me[axis] < sizes[axis] - 1 if side == LOW else me[axis] > 0

    def receives(axis, side):
        return me[axis] > 0 if side == LOW else me[axis] < sizes[axis] - 1

    def y_copy(slot, side):
        return remote(
            ysend.at[slot, side],
            yrecv.at[slot, side],
            ys_sem.at[slot, side],
            yr_sem.at[slot, side],
            1,
            target_of(1, side),
        )

    def z_copy(slot, side, c):
        x = pl.ds(1, nx)
        rows = pl.ds(PY + c * chunk, chunk)
        source, land = (nz, 0) if side == LOW else (PZ, PZ + nz)
        return remote(
            d.at[slot, x, rows, pl.ds(source, PZ)],
            d.at[slot, x, rows, pl.ds(land, PZ)],
            zs_sem.at[slot, side, c],
            zr_sem.at[slot, side, c],
            2,
            target_of(2, side),
        )

    def open_each(slot, c, act):
        rule = receives if act == "wait_recv" else sends
        for side in (LOW, HIGH):
            row_in = CHUNKS - 1 if side == LOW and act != "wait_recv" else 0

            @pl.when(rule(2, side))
            def _(side=side):
                getattr(z_copy(slot, side, c), act)()

            if c == row_in:
                @pl.when(rule(1, side))
                def _(side=side):
                    getattr(y_copy(slot, side), act)()

    def pack(slot, x, c):
        if c == CHUNKS - 1:
            ysend[slot, LOW, x - 1] = d[slot, x, pl.ds(PY + ny - 1, 1), mid_z]
        if c == 0:
            ysend[slot, HIGH, x - 1] = d[slot, x, pl.ds(PY, 1), mid_z]

    def unpack(slot, x, c):
        if c == 0:
            d[slot, x, pl.ds(PY - 1, 1), mid_z] = yrecv[slot, LOW, x - 1]
        if c == CHUNKS - 1:
            d[slot, x, pl.ds(PY + ny, 1), mid_z] = yrecv[slot, HIGH, x - 1]

    def block(k, x, y):
        slot, other = k % 2, (k + 1) % 2
        here = (x - 1, pl.ds(y, ROWS), slice(None))
        rows = pl.ds(PY + y, ROWS)
        mid = d[slot, x, rows, mid_z]
        px = d[slot, x + 1, rows, mid_z]
        mx = d[slot, x - 1, rows, mid_z]
        py = d[slot, x, pl.ds(PY + y + 1, ROWS), mid_z]
        my = d[slot, x, pl.ds(PY + y - 1, ROWS), mid_z]
        wide = nz + PZ
        pz = pltpu.roll(d[slot, x, rows, pl.ds(PZ, wide)], wide - 1, 1)[:, :nz]
        mz = pltpu.roll(d[slot, x, rows, pl.ds(0, wide)], 1, 1)[:, PZ:]
        beside = ((px + mx) + (py + my)) + (pz + mz)
        skew = vel[0, *here] * (px - mx) + vel[1, *here] * (py - my)
        skew = skew + vel[2, *here] * (pz - mz)
        applied = (6.0 + reac[here]) * mid - (beside - skew)
        if k == 0:
            left = mid - (1.0 / centre) * applied
            sol[here] = (1.0 / centre) * mid
        else:
            left = res[here] - applied
            sol[here] = sol[here] + mid
        res[here] = left
        if k + 1 < ITERS:
            keep = weights[k + 1] * weights[k] * (1.0 / centre if k == 0 else 1.0)
            d[other, x, rows, mid_z] = keep * mid + (
                2.0 * weights[k + 1] / half_width
            ) * left
            return None
        return left * left

    def add(total, term):
        return total if term is None else total + term

    load_rhs[0].wait()
    load_rhs[1].wait()
    for c in order:
        for side in (LOW, HIGH):
            x_copy(0, side, c).start()
    load_rhs[2].wait()

    def pack_first(x, carry):
        for c in (0, CHUNKS - 1):
            pack(0, x, c)
        return carry

    lax.fori_loop(1, nx + 1, pack_first, 0)
    for c in order:
        open_each(0, c, "start")

    total = jnp.zeros((ROWS, nz), jnp.float32)
    for k in range(ITERS):
        slot, other = k % 2, (k + 1) % 2
        more = k + 1 < ITERS
        for c in order:
            if k == 0:
                for copy in loads[c]:
                    copy.wait()
            open_each(slot, c, "wait_recv")
            if k > 0:
                open_each(other, c, "wait_send")
                for side in (LOW, HIGH):
                    x_copy(other, side, c).wait_send()

            def planes(xs, total, k=k, c=c, slot=slot, other=other, more=more):
                for x in xs:
                    unpack(slot, x, c)
                for x in xs:
                    for y in range(c * chunk, (c + 1) * chunk, ROWS):
                        total = add(total, block(k, x, y))
                if more:
                    for x in xs:
                        pack(other, x, c)
                return total

            def group(i, total, planes=planes):
                return planes([2 + i * GROUP + j for j in range(GROUP)], total)

            total = lax.fori_loop(0, (nx - 2) // GROUP, group, total)
            for side in (LOW, HIGH):
                x_copy(slot, side, c).wait_recv()
            total = planes((1, nx), total)
            if more:
                for side in (LOW, HIGH):
                    x_copy(other, side, c).start()
                open_each(other, c, "start")

    tile = total[:, :PZ]
    for z in range(PZ, nz, PZ):
        tile = tile + total[:, z : z + PZ]
    tile = jnp.sum(tile, axis=0, keepdims=True)
    first = 0
    for axes in phases(sizes):
        group = phase_steps(sizes, axes)
        own = jnp.int32(0)
        for axis in axes:
            own = own * sizes[axis] + me[axis]
        part[first + own] = tile
        copies = [
            pltpu.make_async_remote_copy(
                src_ref=part.at[first + own],
                dst_ref=part.at[first + own],
                send_sem=ps_sem.at[first + p],
                recv_sem=pr_sem.at[first + p],
                device_id=shifted(steps),
                device_id_type=pl.DeviceIdType.MESH,
            )
            for p, steps in enumerate(group)
        ]
        for copy in copies:
            copy.start()
        for copy in copies:
            copy.wait_recv()
        tile = part[first]
        for p in range(1, len(group) + 1):
            tile = tile + part[first + p]
        for copy in copies:
            copy.wait_send()
        first += len(group) + 1
    last = (ITERS - 1) % 2
    for c in order:
        open_each(last, c, "wait_send")
        for side in (LOW, HIGH):
            x_copy(last, side, c).wait_send()
    cells = nx * ny * nz * sizes[0] * sizes[1] * sizes[2]
    mean = jnp.sum(tile, keepdims=True) / cells
    norm[...] = jnp.sqrt(mean + 1e-06)


def put_out(sol, res, sol_out, res_out, sem):
    part = sol.shape[0] // 4
    copies = [
        pltpu.make_async_copy(
            source.at[pl.ds(i * part, part)],
            target.at[pl.ds(i * part, part)],
            sem.at[j, i],
        )
        for i in range(4)
        for j, (source, target) in enumerate(((sol, sol_out), (res, res_out)))
    ]
    for copy in copies:
        copy.start()
    for copy in copies:
        copy.wait()


def local(sizes, right_side, reaction, velocity):
    nx, ny, nz = right_side.shape
    hbm = pl.BlockSpec(memory_space=pltpu.HBM)
    vmem = pl.BlockSpec(memory_space=pltpu.VMEM)
    dma = pltpu.SemaphoreType.DMA
    field = jax.ShapeDtypeStruct((nx, ny, nz), jnp.float32)
    sol, res, norm = pl.pallas_call(
        functools.partial(kernel, sizes),
        out_shape=(field, field, jax.ShapeDtypeStruct((1, 1), jnp.float32)),
        in_specs=[hbm] * 3,
        out_specs=(vmem, vmem, vmem),
        scratch_shapes=[
            pltpu.VMEM((2, nx + 2, ny + 2 * PY, nz + 2 * PZ), jnp.float32),
            pltpu.VMEM((nx, ny, nz), jnp.float32),
            pltpu.VMEM((3, nx, ny, nz), jnp.float32),
            pltpu.VMEM((2, 2, nx, 1, nz), jnp.float32),
            pltpu.VMEM((2, 2, nx, 1, nz), jnp.float32),
            pltpu.VMEM((phase_slots(sizes), 1, PZ), jnp.float32),
            dma((3,)),
            dma((CHUNKS, 2)),
            dma((2, 2, CHUNKS)),
            dma((2, 2, CHUNKS)),
            dma((2, 2)),
            dma((2, 2)),
            dma((2, 2, CHUNKS)),
            dma((2, 2, CHUNKS)),
            dma((phase_slots(sizes),)),
            dma((phase_slots(sizes),)),
        ],
        compiler_params=pltpu.CompilerParams(
            collective_id=0,
            has_side_effects=True,
            vmem_limit_bytes=40 * 1024 * 1024,
        ),
    )(
        *(
            pltpu.with_memory_space_constraint(a, pltpu.HBM)
            for a in (right_side, reaction, velocity)
        )
    )
    sol, res = pl.pallas_call(
        put_out,
        out_shape=(field, field),
        in_specs=[vmem] * 2,
        out_specs=(hbm, hbm),
        scratch_shapes=[dma((2, 4))],
        compiler_params=pltpu.CompilerParams(vmem_limit_bytes=16 * 1024 * 1024),
    )(sol, res)
    return sol, res, norm[0, 0]


def solution(mesh):
    sizes = tuple(mesh.shape[a] for a in AXES)
    return jax.shard_map(
        functools.partial(local, sizes),
        mesh=mesh,
        in_specs=(P("gx", "gy", "gz"), P("gx", "gy", "gz"), P(None, "gx", "gy", "gz")),
        out_specs=(P("gx", "gy", "gz"), P("gx", "gy", "gz"), P()),
        check_vma=False,
    )
```

```python
import functools
import itertools

import jax
import jax.numpy as jnp
from jax import lax
from jax.experimental import pallas as pl
from jax.experimental.pallas import tpu as pltpu
from jax.sharding import PartitionSpec as P

ITERS = 5
CHUNKS = 4
ROWS = 8
GROUP = 7

centre = 7.25
half_width = 6.75

AXES = ("gx", "gy", "gz")
PY, PZ = 8, 128
LOW, HIGH = 0, 1


def chebyshev_weights(count):
    ratio_value = centre / half_width
    weights = [1.0 / ratio_value]
    for iteration in range(count):
        weights.append(1.0 / (2.0 * ratio_value - weights[-1]))
    return weights


def reaches(sizes):
    return sizes[0] // 2 + sizes[1] - 1 + sizes[2] - 1 <= ITERS + 1


def phases(sizes):
    return ((0, 1, 2),) if reaches(sizes) else ((2,), (0, 1))


def phase_steps(sizes, axes):
    ranges = [range(n) if i in axes else (0,) for i, n in enumerate(sizes)]
    return [steps for steps in itertools.product(*ranges) if any(steps)]


def greeted_by(sizes):
    steps = {
        tuple(p if j == i else 0 for j in range(len(sizes)))
        for i, n in enumerate(sizes)
        for p in (1, n - 1)
    }
    for axes in phases(sizes):
        steps |= set(phase_steps(sizes, axes))
    return sorted(steps)


def phase_slots(sizes):
    return sum(len(phase_steps(sizes, axes)) + 1 for axes in phases(sizes))


def kernel(
    sizes,
    rhs,
    reaction,
    velocity,
    sol,
    res,
    norm,
    d,
    coef,
    ysend,
    yrecv,
    part,
    rhs_sem,
    load_sem,
    xs_sem,
    xr_sem,
    ys_sem,
    yr_sem,
    zs_sem,
    zr_sem,
    ps_sem,
    pr_sem,
):
    nx, ny, nz = rhs.shape
    weights = chebyshev_weights(ITERS)
    me = [lax.axis_index(a) for a in AXES]
    mid_y = pl.ds(PY, ny)
    mid_z = pl.ds(PZ, nz)
    chunk = ny // CHUNKS

    barrier = pltpu.get_barrier_semaphore()
    def shifted(steps):
        return {
            a: lax.rem(i + p, n)
            for a, n, i, p in zip(AXES, sizes, me, steps)
            if p
        }

    def greet(steps):
        pl.semaphore_signal(
            barrier,
            inc=1,
            device_id=shifted(steps),
            device_id_type=pl.DeviceIdType.MESH,
        )

    if reaches(sizes):
        for step in sorted({1, sizes[0] - 1}):
            greet((step, 0, 0))
        greeters = len({1, sizes[0] - 1})
        for axis in (1, 2):
            for step, there in (
                (1, me[axis] < sizes[axis] - 1),
                (sizes[axis] - 1, me[axis] > 0),
            ):
                @pl.when(there)
                def _(axis=axis, step=step):
                    greet(tuple(step if a == axis else 0 for a in range(3)))

                greeters = greeters + there.astype(jnp.int32)
    else:
        for steps in greeted_by(sizes):
            greet(steps)
        greeters = len(greeted_by(sizes))

    order = [0, CHUNKS - 1] + list(range(1, CHUNKS - 1))
    load_rhs = [
        pltpu.make_async_copy(
            rhs.at[pl.ds(first, count)],
            d.at[0, pl.ds(1 + first, count), mid_y, mid_z],
            rhs_sem.at[i],
        )
        for i, (first, count) in enumerate(((0, 1), (nx - 1, 1), (1, nx - 2)))
    ]
    loads = {}
    for c in order:
        rows = pl.ds(c * chunk, chunk)
        loads[c] = [
            pltpu.make_async_copy(
                reaction.at[:, rows], coef.at[3, :, rows], load_sem.at[c]
            ),
            pltpu.make_async_copy(
                velocity.at[:, :, rows],
                coef.at[pl.ds(0, 3), :, rows],
                load_sem.at[c],
            ),
        ]
    for copy in load_rhs:
        copy.start()
    for c in order:
        for copy in loads[c]:
            copy.start()

    for side, at_edge in ((LOW, me[1] == 0), (HIGH, me[1] == sizes[1] - 1)):
        @pl.when(at_edge)
        def _(side=side):
            for slot in range(2):
                yrecv[slot, side] = jnp.zeros((nx, 1, nz), jnp.float32)

    for first, at_edge in ((0, me[2] == 0), (PZ + nz, me[2] == sizes[2] - 1)):
        @pl.when(at_edge)
        def _(first=first):
            def clear(x, carry):
                for slot in range(2):
                    d[slot, x, pl.ds(PY, ny), pl.ds(first, PZ)] = jnp.zeros(
                        (ny, PZ), jnp.float32
                    )
                return carry

            lax.fori_loop(1, nx + 1, clear, 0)

    pl.semaphore_wait(barrier, greeters)

    def remote(src, dst, send, recv, axis, target):
        return pltpu.make_async_remote_copy(
            src_ref=src,
            dst_ref=dst,
            send_sem=send,
            recv_sem=recv,
            device_id={AXES[axis]: target},
            device_id_type=pl.DeviceIdType.MESH,
        )

    def x_copy(slot, side, c):
        n = sizes[0]
        rows = pl.ds(PY + c * chunk, chunk)
        plane, land, target = (
            (nx, 0, lax.rem(me[0] + 1, n))
            if side == LOW
            else (1, nx + 1, lax.rem(me[0] + n - 1, n))
        )
        return remote(
            d.at[slot, plane, rows, mid_z],
            d.at[slot, land, rows, mid_z],
            xs_sem.at[slot],
            xr_sem.at[slot, side, c],
            0,
            target,
        )

    def start_x(slot, c):
        for even, sides in ((True, (HIGH, LOW)), (False, (LOW, HIGH))):
            @pl.when((lax.rem(me[0], 2) == 0) == even)
            def _(sides=sides):
                for side in sides:
                    x_copy(slot, side, c).start()

    def target_of(axis, side):
        n = sizes[axis]
        step = 1 if side == LOW else n - 1
        return lax.rem(me[axis] + step, n)

    def sends(axis, side):
        return me[axis] < sizes[axis] - 1 if side == LOW else me[axis] > 0

    def receives(axis, side):
        return me[axis] > 0 if side == LOW else me[axis] < sizes[axis] - 1

    def y_copy(slot, side):
        return remote(
            ysend.at[slot, side],
            yrecv.at[slot, side],
            ys_sem.at[slot, side],
            yr_sem.at[slot, side],
            1,
            target_of(1, side),
        )

    def z_copy(slot, side, c):
        x = pl.ds(1, nx)
        rows = pl.ds(PY + c * chunk, chunk)
        source, land = (nz, 0) if side == LOW else (PZ, PZ + nz)
        return remote(
            d.at[slot, x, rows, pl.ds(source, PZ)],
            d.at[slot, x, rows, pl.ds(land, PZ)],
            zs_sem.at[slot, side],
            zr_sem.at[slot, side, c],
            2,
            target_of(2, side),
        )

    def sent(slot):
        both = d.at[slot, pl.ds(0, 2), mid_y, mid_z]
        remote(both, both, xs_sem.at[slot], xr_sem.at[slot, 0, 0], 0, me[0]).wait_send()
        for side in (LOW, HIGH):
            @pl.when(sends(2, side))
            def _(side=side):
                edge = d.at[slot, pl.ds(1, nx), mid_y, pl.ds(0, PZ)]
                remote(
                    edge, edge, zs_sem.at[slot, side], zr_sem.at[slot, side, 0], 2, me[2]
                ).wait_send()

            @pl.when(sends(1, side))
            def _(side=side):
                y_copy(slot, side).wait_send()

    def open_each(slot, c, act):
        rule = receives if act == "wait_recv" else sends
        for side in (LOW, HIGH):
            row_in = CHUNKS - 1 if side == LOW and act != "wait_recv" else 0

            @pl.when(rule(2, side))
            def _(side=side):
                getattr(z_copy(slot, side, c), act)()

            if c == row_in:
                @pl.when(rule(1, side))
                def _(side=side):
                    getattr(y_copy(slot, side), act)()

    def pack(slot, x, c):
        if c == CHUNKS - 1:
            ysend[slot, LOW, x - 1] = d[slot, x, pl.ds(PY + ny - 1, 1), mid_z]
        if c == 0:
            ysend[slot, HIGH, x - 1] = d[slot, x, pl.ds(PY, 1), mid_z]

    def unpack(slot, x, c):
        if c == 0:
            d[slot, x, pl.ds(PY - 1, 1), mid_z] = yrecv[slot, LOW, x - 1]
        if c == CHUNKS - 1:
            d[slot, x, pl.ds(PY + ny, 1), mid_z] = yrecv[slot, HIGH, x - 1]

    def block(k, x, y):
        slot, other = k % 2, (k + 1) % 2
        here = (x - 1, pl.ds(y, ROWS), slice(None))
        rows = pl.ds(PY + y, ROWS)
        mid = d[slot, x, rows, mid_z]
        px = d[slot, x + 1, rows, mid_z]
        mx = d[slot, x - 1, rows, mid_z]
        py = d[slot, x, pl.ds(PY + y + 1, ROWS), mid_z]
        my = d[slot, x, pl.ds(PY + y - 1, ROWS), mid_z]
        wide = nz + PZ
        pz = pltpu.roll(d[slot, x, rows, pl.ds(PZ, wide)], wide - 1, 1)[:, :nz]
        mz = pltpu.roll(d[slot, x, rows, pl.ds(0, wide)], 1, 1)[:, PZ:]
        beside = ((px + mx) + (py + my)) + (pz + mz)
        skew = coef[0, *here] * (px - mx) + coef[1, *here] * (py - my)
        skew = skew + coef[2, *here] * (pz - mz)
        applied = (6.0 + coef[3, *here]) * mid - (beside - skew)
        if k == 0:
            left = mid - (1.0 / centre) * applied
            sol[here] = (1.0 / centre) * mid
        else:
            left = res[here] - applied
            sol[here] = sol[here] + mid
        res[here] = left
        if k + 1 < ITERS:
            keep = weights[k + 1] * weights[k] * (1.0 / centre if k == 0 else 1.0)
            d[other, x, rows, mid_z] = keep * mid + (
                2.0 * weights[k + 1] / half_width
            ) * left
            return None
        return left * left

    def add(total, term):
        return total if term is None else total + term

    load_rhs[0].wait()
    load_rhs[1].wait()
    for c in order:
        start_x(0, c)
    load_rhs[2].wait()

    def pack_first(x, carry):
        for c in (0, CHUNKS - 1):
            pack(0, x, c)
        return carry

    lax.fori_loop(1, nx + 1, pack_first, 0)
    for c in order:
        open_each(0, c, "start")

    total = jnp.zeros((ROWS, nz), jnp.float32)
    for k in range(ITERS):
        slot, other = k % 2, (k + 1) % 2
        more = k + 1 < ITERS
        for c in order:
            if k == 0:
                block_of = coef.at[:, :, pl.ds(c * chunk, chunk)]
                pltpu.make_async_copy(block_of, block_of, load_sem.at[c]).wait()
            open_each(slot, c, "wait_recv")
            if k > 0 and c == order[0]:
                sent(other)

            def planes(xs, total, k=k, c=c, slot=slot, other=other, more=more):
                for x in xs:
                    unpack(slot, x, c)
                for x in xs:
                    for y in range(c * chunk, (c + 1) * chunk, ROWS):
                        total = add(total, block(k, x, y))
                if more:
                    for x in xs:
                        pack(other, x, c)
                return total

            def group(i, total, planes=planes):
                return planes([2 + i * GROUP + j for j in range(GROUP)], total)

            total = lax.fori_loop(0, (nx - 2) // GROUP, group, total)
            for side in (LOW, HIGH):
                x_copy(slot, side, c).wait_recv()
            total = planes((1, nx), total)
            if more:
                start_x(other, c)
                open_each(other, c, "start")

    tile = total[:, :PZ]
    for z in range(PZ, nz, PZ):
        tile = tile + total[:, z : z + PZ]
    tile = jnp.sum(tile, axis=0, keepdims=True)
    first = 0
    for phase, axes in enumerate(phases(sizes)):
        group = phase_steps(sizes, axes)
        own = jnp.int32(0)
        for axis in axes:
            own = own * sizes[axis] + me[axis]
        part[first + own] = tile

        def message(source, steps):
            return pltpu.make_async_remote_copy(
                src_ref=source,
                dst_ref=source,
                send_sem=ps_sem.at[phase],
                recv_sem=pr_sem.at[phase],
                device_id=shifted(steps),
                device_id_type=pl.DeviceIdType.MESH,
            )

        for steps in group:
            message(part.at[first + own], steps).start()
        whole = message(part.at[pl.ds(first, len(group))], group[0])
        if phase == 0:
            sent((ITERS - 1) % 2)
        whole.wait_send()
        whole.wait_recv()
        tile = part[first]
        for p in range(1, len(group) + 1):
            tile = tile + part[first + p]
        first += len(group) + 1
    cells = nx * ny * nz * sizes[0] * sizes[1] * sizes[2]
    mean = jnp.sum(tile, keepdims=True) / cells
    norm[...] = jnp.broadcast_to(jnp.sqrt(mean + 1e-06), norm.shape)


def put_out(sol, res, norm, sol_out, res_out, norm_out, sem):
    copies = [
        pltpu.make_async_copy(source, target, sem.at[i])
        for i, (source, target) in enumerate(
            ((sol, sol_out), (res, res_out), (norm, norm_out))
        )
    ]
    for copy in copies:
        copy.start()
    for copy in copies:
        copy.wait()


def local(sizes, right_side, reaction, velocity):
    nx, ny, nz = right_side.shape
    hbm = pl.BlockSpec(memory_space=pltpu.HBM)
    vmem = pl.BlockSpec(memory_space=pltpu.VMEM)
    dma = pltpu.SemaphoreType.DMA
    field = jax.ShapeDtypeStruct((nx, ny, nz), jnp.float32)
    sol, res, norm = pl.pallas_call(
        functools.partial(kernel, sizes),
        out_shape=(field, field, jax.ShapeDtypeStruct((1, PZ), jnp.float32)),
        in_specs=[hbm] * 3,
        out_specs=(vmem, vmem, vmem),
        scratch_shapes=[
            pltpu.VMEM((2, nx + 2, ny + 2 * PY, nz + 2 * PZ), jnp.float32),
            pltpu.VMEM((4, nx, ny, nz), jnp.float32),
            pltpu.VMEM((2, 2, nx, 1, nz), jnp.float32),
            pltpu.VMEM((2, 2, nx, 1, nz), jnp.float32),
            pltpu.VMEM((phase_slots(sizes), 1, PZ), jnp.float32),
            dma((3,)),
            dma((CHUNKS,)),
            dma((2,)),
            dma((2, 2, CHUNKS)),
            dma((2, 2)),
            dma((2, 2)),
            dma((2, 2)),
            dma((2, 2, CHUNKS)),
            dma((len(phases(sizes)),)),
            dma((len(phases(sizes)),)),
        ],
        compiler_params=pltpu.CompilerParams(
            collective_id=0,
            has_side_effects=True,
            vmem_limit_bytes=40 * 1024 * 1024,
        ),
    )(
        *(
            pltpu.with_memory_space_constraint(a, pltpu.HBM)
            for a in (right_side, reaction, velocity)
        )
    )
    sol, res, norm = pl.pallas_call(
        put_out,
        out_shape=(field, field, jax.ShapeDtypeStruct((1, PZ), jnp.float32)),
        in_specs=[vmem] * 3,
        out_specs=(hbm,) * 3,
        scratch_shapes=[dma((3,))],
        compiler_params=pltpu.CompilerParams(vmem_limit_bytes=16 * 1024 * 1024),
    )(sol, res, norm)
    return sol, res, norm[0, 0]


def solution(mesh):
    sizes = tuple(mesh.shape[a] for a in AXES)
    return jax.shard_map(
        functools.partial(local, sizes),
        mesh=mesh,
        in_specs=(P("gx", "gy", "gz"), P("gx", "gy", "gz"), P(None, "gx", "gy", "gz")),
        out_specs=(P("gx", "gy", "gz"), P("gx", "gy", "gz"), P()),
        check_vma=False,
    )
```

```python
import functools
import itertools

import jax
import jax.numpy as jnp
from jax import lax
from jax.experimental import pallas as pl
from jax.experimental.pallas import tpu as pltpu
from jax.sharding import PartitionSpec as P

ITERS = 5
CHUNKS = 3
FIRST, LAST = 0, 1
ROWS = 8
GROUP = 7
EDGE = 2

centre = 7.25
half_width = 6.75

AXES = ("gx", "gy", "gz")
PY, PZ = 8, 128
LOW, HIGH = 0, 1


def row_chunks(ny):
    edge = EDGE * (ny // ROWS) // 8 * ROWS
    return [(0, edge), (ny - edge, edge), (edge, ny - 2 * edge)]


def chebyshev_weights(count):
    ratio_value = centre / half_width
    weights = [1.0 / ratio_value]
    for iteration in range(count):
        weights.append(1.0 / (2.0 * ratio_value - weights[-1]))
    return weights


def reaches(sizes):
    return sizes[0] // 2 + sizes[1] - 1 + sizes[2] - 1 <= ITERS + 1


def phases(sizes):
    return ((0, 1, 2),) if reaches(sizes) else ((2,), (0, 1))


def phase_steps(sizes, axes):
    ranges = [range(n) if i in axes else (0,) for i, n in enumerate(sizes)]
    found = [steps for steps in itertools.product(*ranges) if any(steps)]
    hops = lambda steps: min(steps[0], sizes[0] - steps[0]) + sum(steps[1:])
    return sorted(found, key=hops, reverse=True)


def greeted_by(sizes):
    steps = {
        tuple(p if j == i else 0 for j in range(len(sizes)))
        for i, n in enumerate(sizes)
        for p in (1, n - 1)
    }
    for axes in phases(sizes):
        steps |= set(phase_steps(sizes, axes))
    return sorted(steps)


def phase_slots(sizes):
    return sum(len(phase_steps(sizes, axes)) + 1 for axes in phases(sizes))


def kernel(
    sizes,
    rhs,
    reaction,
    velocity,
    sol,
    res,
    sums,
    d,
    coef,
    ysend,
    yrecv,
    part,
    rhs_sem,
    load_sem,
    xs_sem,
    xr_sem,
    ys_sem,
    yr_sem,
    zs_sem,
    zr_sem,
    ps_sem,
    pr_sem,
):
    nx, ny, nz = rhs.shape
    weights = chebyshev_weights(ITERS)
    me = [lax.axis_index(a) for a in AXES]
    mid_y = pl.ds(PY, ny)
    mid_z = pl.ds(PZ, nz)
    chunks = row_chunks(ny)

    barrier = pltpu.get_barrier_semaphore()
    def shifted(steps):
        return {
            a: lax.rem(i + p, n)
            for a, n, i, p in zip(AXES, sizes, me, steps)
            if p
        }

    def greet(steps):
        pl.semaphore_signal(
            barrier,
            inc=1,
            device_id=shifted(steps),
            device_id_type=pl.DeviceIdType.MESH,
        )

    if reaches(sizes):
        for step in sorted({1, sizes[0] - 1}):
            greet((step, 0, 0))
        greeters = len({1, sizes[0] - 1})
        for axis in (1, 2):
            for step, there in (
                (1, me[axis] < sizes[axis] - 1),
                (sizes[axis] - 1, me[axis] > 0),
            ):
                @pl.when(there)
                def _(axis=axis, step=step):
                    greet(tuple(step if a == axis else 0 for a in range(3)))

                greeters = greeters + there.astype(jnp.int32)
    else:
        for steps in greeted_by(sizes):
            greet(steps)
        greeters = len(greeted_by(sizes))

    order = range(CHUNKS)
    load_rhs = [
        pltpu.make_async_copy(
            rhs.at[pl.ds(first, count)],
            d.at[0, pl.ds(1 + first, count), mid_y, mid_z],
            rhs_sem.at[i // 2],
        )
        for i, (first, count) in enumerate(((0, 1), (nx - 1, 1), (1, nx - 2)))
    ]
    loads = {}
    for c in order:
        rows = pl.ds(*chunks[c])
        loads[c] = [
            pltpu.make_async_copy(
                reaction.at[:, rows], coef.at[3, :, rows], load_sem.at[c]
            ),
            pltpu.make_async_copy(
                velocity.at[:, :, rows],
                coef.at[pl.ds(0, 3), :, rows],
                load_sem.at[c],
            ),
        ]
    for copy in load_rhs:
        copy.start()
    for c in order:
        for copy in loads[c]:
            copy.start()

    for side, at_edge in ((LOW, me[1] == 0), (HIGH, me[1] == sizes[1] - 1)):
        @pl.when(at_edge)
        def _(side=side):
            for slot in range(2):
                yrecv[slot, side] = jnp.zeros((nx, 1, nz), jnp.float32)

    for first, at_edge in ((0, me[2] == 0), (PZ + nz, me[2] == sizes[2] - 1)):
        @pl.when(at_edge)
        def _(first=first):
            def clear(x, carry):
                for slot in range(2):
                    d[slot, x, pl.ds(PY, ny), pl.ds(first, PZ)] = jnp.zeros(
                        (ny, PZ), jnp.float32
                    )
                return carry

            lax.fori_loop(1, nx + 1, clear, 0)

    pl.semaphore_wait(barrier, greeters)

    def remote(src, dst, send, recv, axis, target):
        return pltpu.make_async_remote_copy(
            src_ref=src,
            dst_ref=dst,
            send_sem=send,
            recv_sem=recv,
            device_id={AXES[axis]: target},
            device_id_type=pl.DeviceIdType.MESH,
        )

    def x_copy(slot, side, c):
        n = sizes[0]
        rows = pl.ds(PY + chunks[c][0], chunks[c][1])
        plane, land, target = (
            (nx, 0, lax.rem(me[0] + 1, n))
            if side == LOW
            else (1, nx + 1, lax.rem(me[0] + n - 1, n))
        )
        return remote(
            d.at[slot, plane, rows, mid_z],
            d.at[slot, land, rows, mid_z],
            xs_sem.at[slot],
            xr_sem.at[slot, side, c],
            0,
            target,
        )

    def start_x(slot, c):
        for even, sides in ((True, (HIGH, LOW)), (False, (LOW, HIGH))):
            @pl.when((lax.rem(me[0], 2) == 0) == even)
            def _(sides=sides):
                for side in sides:
                    x_copy(slot, side, c).start()

    def target_of(axis, side):
        n = sizes[axis]
        step = 1 if side == LOW else n - 1
        return lax.rem(me[axis] + step, n)

    def sends(axis, side):
        return me[axis] < sizes[axis] - 1 if side == LOW else me[axis] > 0

    def receives(axis, side):
        return me[axis] > 0 if side == LOW else me[axis] < sizes[axis] - 1

    def y_copy(slot, side):
        return remote(
            ysend.at[slot, side],
            yrecv.at[slot, side],
            ys_sem.at[slot, side],
            yr_sem.at[slot, side],
            1,
            target_of(1, side),
        )

    def z_copy(slot, side, c):
        x = pl.ds(1, nx)
        rows = pl.ds(PY + chunks[c][0], chunks[c][1])
        source, land = (nz, 0) if side == LOW else (PZ, PZ + nz)
        return remote(
            d.at[slot, x, rows, pl.ds(source, PZ)],
            d.at[slot, x, rows, pl.ds(land, PZ)],
            zs_sem.at[slot, side],
            zr_sem.at[slot, side, c],
            2,
            target_of(2, side),
        )

    def sent(slot):
        both = d.at[slot, pl.ds(0, 2), mid_y, mid_z]
        remote(both, both, xs_sem.at[slot], xr_sem.at[slot, 0, 0], 0, me[0]).wait_send()
        for side in (LOW, HIGH):
            @pl.when(sends(2, side))
            def _(side=side):
                edge = d.at[slot, pl.ds(1, nx), mid_y, pl.ds(0, PZ)]
                remote(
                    edge, edge, zs_sem.at[slot, side], zr_sem.at[slot, side, 0], 2, me[2]
                ).wait_send()

            @pl.when(sends(1, side))
            def _(side=side):
                y_copy(slot, side).wait_send()

    def open_each(slot, c, act):
        rule = receives if act == "wait_recv" else sends
        for side in (LOW, HIGH):
            row_in = LAST if side == LOW and act != "wait_recv" else FIRST

            @pl.when(rule(2, side))
            def _(side=side):
                getattr(z_copy(slot, side, c), act)()

            if c == row_in:
                @pl.when(rule(1, side))
                def _(side=side):
                    getattr(y_copy(slot, side), act)()

    def pack(slot, x, c):
        if c == LAST:
            ysend[slot, LOW, x - 1] = d[slot, x, pl.ds(PY + ny - 1, 1), mid_z]
        if c == FIRST:
            ysend[slot, HIGH, x - 1] = d[slot, x, pl.ds(PY, 1), mid_z]

    def unpack(slot, x, c):
        if c == FIRST:
            d[slot, x, pl.ds(PY - 1, 1), mid_z] = yrecv[slot, LOW, x - 1]
        if c == LAST:
            d[slot, x, pl.ds(PY + ny, 1), mid_z] = yrecv[slot, HIGH, x - 1]

    def block(k, x, y):
        slot, other = k % 2, (k + 1) % 2
        here = (x - 1, pl.ds(y, ROWS), slice(None))
        rows = pl.ds(PY + y, ROWS)
        mid = d[slot, x, rows, mid_z]
        px = d[slot, x + 1, rows, mid_z]
        mx = d[slot, x - 1, rows, mid_z]
        py = d[slot, x, pl.ds(PY + y + 1, ROWS), mid_z]
        my = d[slot, x, pl.ds(PY + y - 1, ROWS), mid_z]
        wide = nz + PZ
        pz = pltpu.roll(d[slot, x, rows, pl.ds(PZ, wide)], wide - 1, 1)[:, :nz]
        mz = pltpu.roll(d[slot, x, rows, pl.ds(0, wide)], 1, 1)[:, PZ:]
        beside = ((px + mx) + (py + my)) + (pz + mz)
        skew = coef[0, *here] * (px - mx) + coef[1, *here] * (py - my)
        skew = skew + coef[2, *here] * (pz - mz)
        applied = (6.0 + coef[3, *here]) * mid - (beside - skew)
        if k == 0:
            left = mid - (1.0 / centre) * applied
            sol[here] = (1.0 / centre) * mid
        else:
            left = res[here] - applied
            sol[here] = sol[here] + mid
        res[here] = left
        if k + 1 < ITERS:
            keep = weights[k + 1] * weights[k] * (1.0 / centre if k == 0 else 1.0)
            d[other, x, rows, mid_z] = keep * mid + (
                2.0 * weights[k + 1] / half_width
            ) * left
            return None
        return left * left

    def add(total, term):
        return total if term is None else total + term

    two = d.at[0, pl.ds(1, 2), mid_y, mid_z]
    pltpu.make_async_copy(two, two, rhs_sem.at[0]).wait()
    for c in order:
        start_x(0, c)
    load_rhs[2].wait()

    def pack_first(x, carry):
        for c in (FIRST, LAST):
            pack(0, x, c)
        return carry

    lax.fori_loop(1, nx + 1, pack_first, 0)
    for c in order:
        open_each(0, c, "start")

    total = jnp.zeros((ROWS, nz), jnp.float32)
    for k in range(ITERS):
        slot, other = k % 2, (k + 1) % 2
        more = k + 1 < ITERS
        for c in order:
            if k == 0:
                block_of = coef.at[:, :, pl.ds(*chunks[c])]
                pltpu.make_async_copy(block_of, block_of, load_sem.at[c]).wait()
            open_each(slot, c, "wait_recv")
            if k > 0 and c == order[0]:
                sent(other)

            def planes(xs, total, k=k, c=c, slot=slot, other=other, more=more):
                for x in xs:
                    unpack(slot, x, c)
                for x in xs:
                    for y in range(chunks[c][0], sum(chunks[c]), ROWS):
                        total = add(total, block(k, x, y))
                if more:
                    for x in xs:
                        pack(other, x, c)
                return total

            def group(i, total, planes=planes):
                return planes([2 + i * GROUP + j for j in range(GROUP)], total)

            total = lax.fori_loop(0, (nx - 2) // GROUP, group, total)
            for side in (LOW, HIGH):
                x_copy(slot, side, c).wait_recv()
            total = planes((1, nx), total)
            if more:
                start_x(other, c)
                open_each(other, c, "start")

    tile = total[:, :PZ]
    for z in range(PZ, nz, PZ):
        tile = tile + total[:, z : z + PZ]
    tile = jnp.sum(tile, axis=0, keepdims=True)
    first = 0
    for phase, axes in enumerate(phases(sizes)):
        group = phase_steps(sizes, axes)
        own = jnp.int32(0)
        for axis in axes:
            own = own * sizes[axis] + me[axis]
        part[first + own] = tile

        def message(source, steps):
            return pltpu.make_async_remote_copy(
                src_ref=source,
                dst_ref=source,
                send_sem=ps_sem.at[phase],
                recv_sem=pr_sem.at[phase],
                device_id=shifted(steps),
                device_id_type=pl.DeviceIdType.MESH,
            )

        for steps in group:
            message(part.at[first + own], steps).start()
        whole = message(part.at[pl.ds(first, len(group))], group[0])
        if phase == 0:
            sent((ITERS - 1) % 2)
        whole.wait_send()
        whole.wait_recv()
        tile = part[first]
        for p in range(1, len(group) + 1):
            tile = tile + part[first + p]
        first += len(group) + 1
    sums[...] = tile


def put_out(cells, sol, res, sums, sol_out, res_out, norm_out, norm, sem):
    copies = [
        pltpu.make_async_copy(source, target, sem.at[i])
        for i, (source, target) in enumerate(
            ((sol, sol_out), (res, res_out), (norm, norm_out))
        )
    ]
    copies[0].start()
    copies[1].start()
    mean = jnp.sum(sums[...], keepdims=True) / cells
    norm[...] = jnp.broadcast_to(jnp.sqrt(mean + 1e-06), norm.shape)
    copies[2].start()
    for copy in copies:
        copy.wait()


def local(sizes, right_side, reaction, velocity):
    nx, ny, nz = right_side.shape
    hbm = pl.BlockSpec(memory_space=pltpu.HBM)
    vmem = pl.BlockSpec(memory_space=pltpu.VMEM)
    dma = pltpu.SemaphoreType.DMA
    field = jax.ShapeDtypeStruct((nx, ny, nz), jnp.float32)
    sol, res, sums = pl.pallas_call(
        functools.partial(kernel, sizes),
        out_shape=(field, field, jax.ShapeDtypeStruct((1, PZ), jnp.float32)),
        in_specs=[hbm] * 3,
        out_specs=(vmem, vmem, vmem),
        scratch_shapes=[
            pltpu.VMEM((2, nx + 2, ny + 2 * PY, nz + 2 * PZ), jnp.float32),
            pltpu.VMEM((4, nx, ny, nz), jnp.float32),
            pltpu.VMEM((2, 2, nx, 1, nz), jnp.float32),
            pltpu.VMEM((2, 2, nx, 1, nz), jnp.float32),
            pltpu.VMEM((phase_slots(sizes), 1, PZ), jnp.float32),
            dma((2,)),
            dma((CHUNKS,)),
            dma((2,)),
            dma((2, 2, CHUNKS)),
            dma((2, 2)),
            dma((2, 2)),
            dma((2, 2)),
            dma((2, 2, CHUNKS)),
            dma((len(phases(sizes)),)),
            dma((len(phases(sizes)),)),
        ],
        compiler_params=pltpu.CompilerParams(
            collective_id=0,
            has_side_effects=True,
            vmem_limit_bytes=40 * 1024 * 1024,
        ),
    )(
        *(
            pltpu.with_memory_space_constraint(a, pltpu.HBM)
            for a in (right_side, reaction, velocity)
        )
    )
    cells = nx * ny * nz * sizes[0] * sizes[1] * sizes[2]
    sol, res, norm = pl.pallas_call(
        functools.partial(put_out, cells),
        out_shape=(field, field, jax.ShapeDtypeStruct((1, PZ), jnp.float32)),
        in_specs=[vmem] * 3,
        out_specs=(hbm,) * 3,
        scratch_shapes=[pltpu.VMEM((1, PZ), jnp.float32), dma((3,))],
        compiler_params=pltpu.CompilerParams(vmem_limit_bytes=16 * 1024 * 1024),
    )(sol, res, sums)
    return sol, res, norm[0, 0]


def solution(mesh):
    sizes = tuple(mesh.shape[a] for a in AXES)
    return jax.shard_map(
        functools.partial(local, sizes),
        mesh=mesh,
        in_specs=(P("gx", "gy", "gz"), P("gx", "gy", "gz"), P(None, "gx", "gy", "gz")),
        out_specs=(P("gx", "gy", "gz"), P("gx", "gy", "gz"), P()),
        check_vma=False,
    )
```

```python
import functools
import itertools

import jax
import jax.numpy as jnp
from jax import lax
from jax.experimental import pallas as pl
from jax.experimental.pallas import tpu as pltpu
from jax.sharding import PartitionSpec as P

ITERS = 5
CHUNKS = 3
FIRST, LAST = 0, 1
ROWS = 8
GROUP = 7
EDGE = 2

centre = 7.25
half_width = 6.75

AXES = ("gx", "gy", "gz")
PY, PZ = 8, 128
LOW, HIGH = 0, 1


def row_chunks(ny):
    edge = EDGE * (ny // ROWS) // 8 * ROWS
    return [(0, edge), (ny - edge, edge), (edge, ny - 2 * edge)]


def chebyshev_weights(count):
    ratio_value = centre / half_width
    weights = [1.0 / ratio_value]
    for iteration in range(count):
        weights.append(1.0 / (2.0 * ratio_value - weights[-1]))
    return weights


def reaches(sizes):
    return sizes[0] // 2 + sizes[1] - 1 + sizes[2] - 1 <= ITERS + 1


def phases(sizes):
    return ((0, 1, 2),) if reaches(sizes) else ((2,), (0, 1))


def phase_steps(sizes, axes):
    ranges = [range(n) if i in axes else (0,) for i, n in enumerate(sizes)]
    found = [steps for steps in itertools.product(*ranges) if any(steps)]
    hops = lambda steps: min(steps[0], sizes[0] - steps[0]) + sum(steps[1:])
    return sorted(found, key=hops, reverse=True)


def greeted_by(sizes):
    steps = {
        tuple(p if j == i else 0 for j in range(len(sizes)))
        for i, n in enumerate(sizes)
        for p in (1, n - 1)
    }
    for axes in phases(sizes):
        steps |= set(phase_steps(sizes, axes))
    return sorted(steps)


def phase_slots(sizes):
    return sum(len(phase_steps(sizes, axes)) + 1 for axes in phases(sizes))


def kernel(
    sizes,
    rhs,
    reaction,
    velocity,
    sol,
    res,
    sums,
    d,
    coef,
    ysend,
    yrecv,
    part,
    rhs_sem,
    load_sem,
    xs_sem,
    xr_sem,
    ys_sem,
    yr_sem,
    zs_sem,
    zr_sem,
    ps_sem,
    pr_sem,
):
    nx, ny, nz = rhs.shape
    weights = chebyshev_weights(ITERS)
    me = [lax.axis_index(a) for a in AXES]
    mid_y = pl.ds(PY, ny)
    mid_z = pl.ds(PZ, nz)
    chunks = row_chunks(ny)

    barrier = pltpu.get_barrier_semaphore()
    def shifted(steps):
        return {
            a: lax.rem(i + p, n)
            for a, n, i, p in zip(AXES, sizes, me, steps)
            if p
        }

    def greet(steps):
        pl.semaphore_signal(
            barrier,
            inc=1,
            device_id=shifted(steps),
            device_id_type=pl.DeviceIdType.MESH,
        )

    if reaches(sizes):
        for step in sorted({1, sizes[0] - 1}):
            greet((step, 0, 0))
        greeters = len({1, sizes[0] - 1})
        for axis in (1, 2):
            for step, there in (
                (1, me[axis] < sizes[axis] - 1),
                (sizes[axis] - 1, me[axis] > 0),
            ):
                @pl.when(there)
                def _(axis=axis, step=step):
                    greet(tuple(step if a == axis else 0 for a in range(3)))

                greeters = greeters + there.astype(jnp.int32)
    else:
        for steps in greeted_by(sizes):
            greet(steps)
        greeters = len(greeted_by(sizes))

    order = range(CHUNKS)

    def landed(c, base=0):
        start, count = chunks[c]
        return pl.ds(base + start, 2 * count if c == FIRST else count)

    load_rhs = [
        pltpu.make_async_copy(
            rhs.at[pl.ds(first, count)],
            d.at[0, pl.ds(1 + first, count), mid_y, mid_z],
            rhs_sem.at[i // 2],
        )
        for i, (first, count) in enumerate(((0, 1), (nx - 1, 1), (1, nx - 2)))
    ]
    loads = {}
    for c in order:
        rows = pl.ds(*chunks[c])
        loads[c] = [
            pltpu.make_async_copy(
                reaction.at[:, rows], coef.at[3, :, rows], load_sem.at[c // 2]
            ),
            pltpu.make_async_copy(
                velocity.at[:, :, rows],
                coef.at[pl.ds(0, 3), :, rows],
                load_sem.at[c // 2],
            ),
        ]
    for copy in load_rhs:
        copy.start()
    for c in order:
        for copy in loads[c]:
            copy.start()

    for side, at_edge in ((LOW, me[1] == 0), (HIGH, me[1] == sizes[1] - 1)):
        @pl.when(at_edge)
        def _(side=side):
            for slot in range(2):
                yrecv[slot, side] = jnp.zeros((nx, 1, nz), jnp.float32)

    for first, at_edge in ((0, me[2] == 0), (PZ + nz, me[2] == sizes[2] - 1)):
        @pl.when(at_edge)
        def _(first=first):
            def clear(x, carry):
                for slot in range(2):
                    d[slot, x, pl.ds(PY, ny), pl.ds(first, PZ)] = jnp.zeros(
                        (ny, PZ), jnp.float32
                    )
                return carry

            lax.fori_loop(1, nx + 1, clear, 0)

    pl.semaphore_wait(barrier, greeters)

    def remote(src, dst, send, recv, axis, target):
        return pltpu.make_async_remote_copy(
            src_ref=src,
            dst_ref=dst,
            send_sem=send,
            recv_sem=recv,
            device_id={AXES[axis]: target},
            device_id_type=pl.DeviceIdType.MESH,
        )

    def x_copy(slot, side, c):
        n = sizes[0]
        rows = pl.ds(PY + chunks[c][0], chunks[c][1])
        plane, land, target = (
            (nx, 0, lax.rem(me[0] + 1, n))
            if side == LOW
            else (1, nx + 1, lax.rem(me[0] + n - 1, n))
        )
        return remote(
            d.at[slot, plane, rows, mid_z],
            d.at[slot, land, rows, mid_z],
            xs_sem.at[slot],
            xr_sem.at[slot, side, c],
            0,
            target,
        )

    def start_x(slot, c):
        for even, sides in ((True, (HIGH, LOW)), (False, (LOW, HIGH))):
            @pl.when((lax.rem(me[0], 2) == 0) == even)
            def _(sides=sides):
                for side in sides:
                    x_copy(slot, side, c).start()

    def target_of(axis, side):
        n = sizes[axis]
        step = 1 if side == LOW else n - 1
        return lax.rem(me[axis] + step, n)

    def sends(axis, side):
        return me[axis] < sizes[axis] - 1 if side == LOW else me[axis] > 0

    def receives(axis, side):
        return me[axis] > 0 if side == LOW else me[axis] < sizes[axis] - 1

    def y_copy(slot, side):
        return remote(
            ysend.at[slot, side],
            yrecv.at[slot, side],
            ys_sem.at[slot, side],
            yr_sem.at[slot, side],
            1,
            target_of(1, side),
        )

    def z_copy(slot, side, c, rows=None):
        x = pl.ds(1, nx)
        rows = pl.ds(PY + chunks[c][0], chunks[c][1]) if rows is None else rows
        source, land = (nz, 0) if side == LOW else (PZ, PZ + nz)
        return remote(
            d.at[slot, x, rows, pl.ds(source, PZ)],
            d.at[slot, x, rows, pl.ds(land, PZ)],
            zs_sem.at[slot, side],
            zr_sem.at[slot, side, c // 2],
            2,
            target_of(2, side),
        )

    def sent(slot):
        both = d.at[slot, pl.ds(0, 2), mid_y, mid_z]
        remote(both, both, xs_sem.at[slot], xr_sem.at[slot, 0, 0], 0, me[0]).wait_send()
        for side in (LOW, HIGH):
            @pl.when(sends(2, side))
            def _(side=side):
                edge = d.at[slot, pl.ds(1, nx), mid_y, pl.ds(0, PZ)]
                remote(
                    edge, edge, zs_sem.at[slot, side], zr_sem.at[slot, side, 0], 2, me[2]
                ).wait_send()

            @pl.when(sends(1, side))
            def _(side=side):
                y_copy(slot, side).wait_send()

    def open_each(slot, c, act):
        rule = receives if act == "wait_recv" else sends
        for side in (LOW, HIGH):
            row_in = LAST if side == LOW and act != "wait_recv" else FIRST

            if act == "start" or c != LAST:
                @pl.when(rule(2, side))
                def _(side=side):
                    rows = None if act == "start" else landed(c, PY)
                    getattr(z_copy(slot, side, c, rows), act)()

            if c == row_in:
                @pl.when(rule(1, side))
                def _(side=side):
                    getattr(y_copy(slot, side), act)()

    def pack(slot, x, c):
        if c == LAST:
            ysend[slot, LOW, x - 1] = d[slot, x, pl.ds(PY + ny - 1, 1), mid_z]
        if c == FIRST:
            ysend[slot, HIGH, x - 1] = d[slot, x, pl.ds(PY, 1), mid_z]

    def unpack(slot, x, c):
        if c == FIRST:
            d[slot, x, pl.ds(PY - 1, 1), mid_z] = yrecv[slot, LOW, x - 1]
        if c == LAST:
            d[slot, x, pl.ds(PY + ny, 1), mid_z] = yrecv[slot, HIGH, x - 1]

    def block(k, x, y):
        slot, other = k % 2, (k + 1) % 2
        here = (x - 1, pl.ds(y, ROWS), slice(None))
        rows = pl.ds(PY + y, ROWS)
        mid = d[slot, x, rows, mid_z]
        px = d[slot, x + 1, rows, mid_z]
        mx = d[slot, x - 1, rows, mid_z]
        py = d[slot, x, pl.ds(PY + y + 1, ROWS), mid_z]
        my = d[slot, x, pl.ds(PY + y - 1, ROWS), mid_z]
        wide = nz + PZ
        pz = pltpu.roll(d[slot, x, rows, pl.ds(PZ, wide)], wide - 1, 1)[:, :nz]
        mz = pltpu.roll(d[slot, x, rows, pl.ds(0, wide)], 1, 1)[:, PZ:]
        beside = ((px + mx) + (py + my)) + (pz + mz)
        skew = coef[0, *here] * (px - mx) + coef[1, *here] * (py - my)
        skew = skew + coef[2, *here] * (pz - mz)
        applied = (6.0 + coef[3, *here]) * mid - (beside - skew)
        if k == 0:
            left = mid - (1.0 / centre) * applied
            sol[here] = (1.0 / centre) * mid
        else:
            left = res[here] - applied
            sol[here] = sol[here] + mid
        res[here] = left
        if k + 1 < ITERS:
            keep = weights[k + 1] * weights[k] * (1.0 / centre if k == 0 else 1.0)
            d[other, x, rows, mid_z] = keep * mid + (
                2.0 * weights[k + 1] / half_width
            ) * left
            return None
        return left * left

    def add(total, term):
        return total if term is None else total + term

    two = d.at[0, pl.ds(1, 2), mid_y, mid_z]
    pltpu.make_async_copy(two, two, rhs_sem.at[0]).wait()
    for c in order:
        start_x(0, c)
    load_rhs[2].wait()

    def pack_first(x, carry):
        for c in (FIRST, LAST):
            pack(0, x, c)
        return carry

    lax.fori_loop(1, nx + 1, pack_first, 0)
    for c in order:
        open_each(0, c, "start")

    total = jnp.zeros((ROWS, nz), jnp.float32)
    for k in range(ITERS):
        slot, other = k % 2, (k + 1) % 2
        more = k + 1 < ITERS
        for c in order:
            if k == 0:
                if c != LAST:
                    block_of = coef.at[:, :, landed(c)]
                    pltpu.make_async_copy(
                        block_of, block_of, load_sem.at[c // 2]
                    ).wait()
            open_each(slot, c, "wait_recv")
            if k > 0 and c == order[0]:
                sent(other)

            def planes(xs, total, k=k, c=c, slot=slot, other=other, more=more):
                for x in xs:
                    unpack(slot, x, c)
                for x in xs:
                    for y in range(chunks[c][0], sum(chunks[c]), ROWS):
                        total = add(total, block(k, x, y))
                if more:
                    for x in xs:
                        pack(other, x, c)
                return total

            def group(i, total, planes=planes):
                return planes([2 + i * GROUP + j for j in range(GROUP)], total)

            total = lax.fori_loop(0, (nx - 2) // GROUP, group, total)
            for side in (LOW, HIGH):
                x_copy(slot, side, c).wait_recv()
            total = planes((1, nx), total)
            if more:
                start_x(other, c)
                open_each(other, c, "start")

    tile = total[:, :PZ]
    for z in range(PZ, nz, PZ):
        tile = tile + total[:, z : z + PZ]
    tile = jnp.sum(tile, axis=0, keepdims=True)
    first = 0
    for phase, axes in enumerate(phases(sizes)):
        group = phase_steps(sizes, axes)
        own = jnp.int32(0)
        for axis in axes:
            own = own * sizes[axis] + me[axis]
        part[first + own] = tile

        def message(source, steps):
            return pltpu.make_async_remote_copy(
                src_ref=source,
                dst_ref=source,
                send_sem=ps_sem.at[phase],
                recv_sem=pr_sem.at[phase],
                device_id=shifted(steps),
                device_id_type=pl.DeviceIdType.MESH,
            )

        for steps in group:
            message(part.at[first + own], steps).start()
        whole = message(part.at[pl.ds(first, len(group))], group[0])
        if phase == 0:
            sent((ITERS - 1) % 2)
        whole.wait_send()
        whole.wait_recv()
        tile = part[first]
        for p in range(1, len(group) + 1):
            tile = tile + part[first + p]
        first += len(group) + 1
    sums[...] = tile


def put_out(cells, sol, res, sums, sol_out, res_out, norm_out, norm, sem):
    copies = [
        pltpu.make_async_copy(source, target, sem.at[i])
        for i, (source, target) in enumerate(
            ((sol, sol_out), (res, res_out), (norm, norm_out))
        )
    ]
    copies[0].start()
    copies[1].start()
    mean = jnp.sum(sums[...], keepdims=True) / cells
    norm[...] = jnp.broadcast_to(jnp.sqrt(mean + 1e-06), norm.shape)
    copies[2].start()
    for copy in copies:
        copy.wait()


def local(sizes, right_side, reaction, velocity):
    nx, ny, nz = right_side.shape
    hbm = pl.BlockSpec(memory_space=pltpu.HBM)
    vmem = pl.BlockSpec(memory_space=pltpu.VMEM)
    dma = pltpu.SemaphoreType.DMA
    field = jax.ShapeDtypeStruct((nx, ny, nz), jnp.float32)
    sol, res, sums = pl.pallas_call(
        functools.partial(kernel, sizes),
        out_shape=(field, field, jax.ShapeDtypeStruct((1, PZ), jnp.float32)),
        in_specs=[hbm] * 3,
        out_specs=(vmem, vmem, vmem),
        scratch_shapes=[
            pltpu.VMEM((2, nx + 2, ny + 2 * PY, nz + 2 * PZ), jnp.float32),
            pltpu.VMEM((4, nx, ny, nz), jnp.float32),
            pltpu.VMEM((2, 2, nx, 1, nz), jnp.float32),
            pltpu.VMEM((2, 2, nx, 1, nz), jnp.float32),
            pltpu.VMEM((phase_slots(sizes), 1, PZ), jnp.float32),
            dma((2,)),
            dma((2,)),
            dma((2,)),
            dma((2, 2, CHUNKS)),
            dma((2, 2)),
            dma((2, 2)),
            dma((2, 2)),
            dma((2, 2, 2)),
            dma((len(phases(sizes)),)),
            dma((len(phases(sizes)),)),
        ],
        compiler_params=pltpu.CompilerParams(
            collective_id=0,
            has_side_effects=True,
            vmem_limit_bytes=40 * 1024 * 1024,
        ),
    )(
        *(
            pltpu.with_memory_space_constraint(a, pltpu.HBM)
            for a in (right_side, reaction, velocity)
        )
    )
    cells = nx * ny * nz * sizes[0] * sizes[1] * sizes[2]
    sol, res, norm = pl.pallas_call(
        functools.partial(put_out, cells),
        out_shape=(field, field, jax.ShapeDtypeStruct((1, PZ), jnp.float32)),
        in_specs=[vmem] * 3,
        out_specs=(hbm,) * 3,
        scratch_shapes=[pltpu.VMEM((1, PZ), jnp.float32), dma((3,))],
        compiler_params=pltpu.CompilerParams(vmem_limit_bytes=16 * 1024 * 1024),
    )(sol, res, sums)
    return sol, res, norm[0, 0]


def solution(mesh):
    sizes = tuple(mesh.shape[a] for a in AXES)
    return jax.shard_map(
        functools.partial(local, sizes),
        mesh=mesh,
        in_specs=(P("gx", "gy", "gz"), P("gx", "gy", "gz"), P(None, "gx", "gy", "gz")),
        out_specs=(P("gx", "gy", "gz"), P("gx", "gy", "gz"), P()),
        check_vma=False,
    )
```

```python
import functools
import itertools

import jax
import jax.numpy as jnp
from jax import lax
from jax.experimental import pallas as pl
from jax.experimental.pallas import tpu as pltpu
from jax.sharding import PartitionSpec as P

ITERS = 5
CHUNKS = 3
FIRST, LAST = 0, 1
ROWS = 8
GROUP = 7
EDGE = 2

centre = 7.25
half_width = 6.75

AXES = ("gx", "gy", "gz")
PY, PZ = 8, 128
LOW, HIGH = 0, 1


def row_chunks(ny):
    edge = EDGE * (ny // ROWS) // 8 * ROWS
    return [(0, edge), (ny - edge, edge), (edge, ny - 2 * edge)]


def chebyshev_weights(count):
    ratio_value = centre / half_width
    weights = [1.0 / ratio_value]
    for iteration in range(count):
        weights.append(1.0 / (2.0 * ratio_value - weights[-1]))
    return weights


def reaches(sizes):
    return sizes[0] // 2 + sizes[1] - 1 + sizes[2] - 1 <= ITERS + 1


def phases(sizes):
    return ((0, 1, 2),) if reaches(sizes) else ((2,), (0, 1))


def phase_steps(sizes, axes):
    ranges = [range(n) if i in axes else (0,) for i, n in enumerate(sizes)]
    found = [steps for steps in itertools.product(*ranges) if any(steps)]
    hops = lambda steps: min(steps[0], sizes[0] - steps[0]) + sum(steps[1:])
    return sorted(found, key=hops, reverse=True)


def greeted_by(sizes):
    steps = {
        tuple(p if j == i else 0 for j in range(len(sizes)))
        for i, n in enumerate(sizes)
        for p in (1, n - 1)
    }
    for axes in phases(sizes):
        steps |= set(phase_steps(sizes, axes))
    return sorted(steps)


def phase_slots(sizes):
    return sum(len(phase_steps(sizes, axes)) + 1 for axes in phases(sizes))


def kernel(
    sizes,
    rhs,
    reaction,
    velocity,
    sol,
    res,
    sums,
    d,
    coef,
    ysend,
    yrecv,
    part,
    rhs_sem,
    load_sem,
    xs_sem,
    xr_sem,
    ys_sem,
    yr_sem,
    zs_sem,
    zr_sem,
    ps_sem,
    pr_sem,
):
    nx, ny, nz = rhs.shape
    weights = chebyshev_weights(ITERS)
    me = [lax.axis_index(a) for a in AXES]
    mid_y = pl.ds(PY, ny)
    mid_z = pl.ds(PZ, nz)
    chunks = row_chunks(ny)

    barrier = pltpu.get_barrier_semaphore()
    def shifted(steps):
        return {
            a: lax.rem(i + p, n)
            for a, n, i, p in zip(AXES, sizes, me, steps)
            if p
        }

    def greet(steps):
        pl.semaphore_signal(
            barrier,
            inc=1,
            device_id=shifted(steps),
            device_id_type=pl.DeviceIdType.MESH,
        )

    if reaches(sizes):
        for step in sorted({1, sizes[0] - 1}):
            greet((step, 0, 0))
        greeters = len({1, sizes[0] - 1})
        for axis in (1, 2):
            for step, there in (
                (1, me[axis] < sizes[axis] - 1),
                (sizes[axis] - 1, me[axis] > 0),
            ):
                @pl.when(there)
                def _(axis=axis, step=step):
                    greet(tuple(step if a == axis else 0 for a in range(3)))

                greeters = greeters + there.astype(jnp.int32)
    else:
        for steps in greeted_by(sizes):
            greet(steps)
        greeters = len(greeted_by(sizes))

    order = range(CHUNKS)

    def landed(c, base=0):
        start, count = chunks[c]
        return pl.ds(base + start, 2 * count if c == FIRST else count)

    load_rhs = [
        pltpu.make_async_copy(
            rhs.at[pl.ds(first, count)],
            d.at[0, pl.ds(1 + first, count), mid_y, mid_z],
            rhs_sem.at[i // 2],
        )
        for i, (first, count) in enumerate(((0, 1), (nx - 1, 1), (1, nx - 2)))
    ]
    loads = {}
    for c in order:
        rows = pl.ds(*chunks[c])
        loads[c] = [
            pltpu.make_async_copy(
                reaction.at[:, rows], coef.at[3, :, rows], load_sem.at[c // 2]
            ),
            pltpu.make_async_copy(
                velocity.at[:, :, rows],
                coef.at[pl.ds(0, 3), :, rows],
                load_sem.at[c // 2],
            ),
        ]
    for copy in load_rhs:
        copy.start()
    for c in order:
        for copy in loads[c]:
            copy.start()

    for side, at_edge in ((LOW, me[1] == 0), (HIGH, me[1] == sizes[1] - 1)):
        @pl.when(at_edge)
        def _(side=side):
            for slot in range(2):
                yrecv[slot, side] = jnp.zeros((nx, 1, nz), jnp.float32)

    for first, at_edge in ((0, me[2] == 0), (PZ + nz, me[2] == sizes[2] - 1)):
        @pl.when(at_edge)
        def _(first=first):
            def clear(x, carry):
                for slot in range(2):
                    d[slot, x, pl.ds(PY, ny), pl.ds(first, PZ)] = jnp.zeros(
                        (ny, PZ), jnp.float32
                    )
                return carry

            lax.fori_loop(1, nx + 1, clear, 0)

    pl.semaphore_wait(barrier, greeters)

    def remote(src, dst, send, recv, axis, target):
        return pltpu.make_async_remote_copy(
            src_ref=src,
            dst_ref=dst,
            send_sem=send,
            recv_sem=recv,
            device_id={AXES[axis]: target},
            device_id_type=pl.DeviceIdType.MESH,
        )

    def x_copy(slot, side, c):
        n = sizes[0]
        rows = pl.ds(PY + chunks[c][0], chunks[c][1])
        plane, land, target = (
            (nx, 0, lax.rem(me[0] + 1, n))
            if side == LOW
            else (1, nx + 1, lax.rem(me[0] + n - 1, n))
        )
        return remote(
            d.at[slot, plane, rows, mid_z],
            d.at[slot, land, rows, mid_z],
            xs_sem.at[slot],
            xr_sem.at[slot, side, c],
            0,
            target,
        )

    def start_x(slot, c):
        for even, sides in ((True, (HIGH, LOW)), (False, (LOW, HIGH))):
            @pl.when((lax.rem(me[0], 2) == 0) == even)
            def _(sides=sides):
                for side in sides:
                    x_copy(slot, side, c).start()

    def target_of(axis, side):
        n = sizes[axis]
        step = 1 if side == LOW else n - 1
        return lax.rem(me[axis] + step, n)

    def sends(axis, side):
        return me[axis] < sizes[axis] - 1 if side == LOW else me[axis] > 0

    def receives(axis, side):
        return me[axis] > 0 if side == LOW else me[axis] < sizes[axis] - 1

    def y_copy(slot, side):
        return remote(
            ysend.at[slot, side],
            yrecv.at[slot, side],
            ys_sem.at[slot, side],
            yr_sem.at[slot, side],
            1,
            target_of(1, side),
        )

    def z_copy(slot, side, c, rows=None):
        x = pl.ds(1, nx)
        rows = pl.ds(PY + chunks[c][0], chunks[c][1]) if rows is None else rows
        source, land = (nz, 0) if side == LOW else (PZ, PZ + nz)
        return remote(
            d.at[slot, x, rows, pl.ds(source, PZ)],
            d.at[slot, x, rows, pl.ds(land, PZ)],
            zs_sem.at[slot],
            zr_sem.at[slot, c // 2],
            2,
            target_of(2, side),
        )

    def sent(slot):
        both = d.at[slot, pl.ds(0, 2), mid_y, mid_z]
        remote(both, both, xs_sem.at[slot], xr_sem.at[slot, 0, 0], 0, me[0]).wait_send()
        for side in (LOW, HIGH):
            @pl.when(sends(2, side))
            def _(side=side):
                edge = d.at[slot, pl.ds(1, nx), mid_y, pl.ds(0, PZ)]
                remote(
                    edge, edge, zs_sem.at[slot], zr_sem.at[slot, 0], 2, me[2]
                ).wait_send()

            @pl.when(sends(1, side))
            def _(side=side):
                y_copy(slot, side).wait_send()

    def open_each(slot, c, act):
        rule = receives if act == "wait_recv" else sends
        for side in (LOW, HIGH):
            row_in = LAST if side == LOW and act != "wait_recv" else FIRST

            if act == "start" or c != LAST:
                @pl.when(rule(2, side))
                def _(side=side):
                    rows = None if act == "start" else landed(c, PY)
                    getattr(z_copy(slot, side, c, rows), act)()

            if c == row_in:
                @pl.when(rule(1, side))
                def _(side=side):
                    getattr(y_copy(slot, side), act)()

    def pack(slot, x, c):
        if c == LAST:
            ysend[slot, LOW, x - 1] = d[slot, x, pl.ds(PY + ny - 1, 1), mid_z]
        if c == FIRST:
            ysend[slot, HIGH, x - 1] = d[slot, x, pl.ds(PY, 1), mid_z]

    def unpack(slot, x, c):
        if c == FIRST:
            d[slot, x, pl.ds(PY - 1, 1), mid_z] = yrecv[slot, LOW, x - 1]
        if c == LAST:
            d[slot, x, pl.ds(PY + ny, 1), mid_z] = yrecv[slot, HIGH, x - 1]

    def block(k, x, y):
        slot, other = k % 2, (k + 1) % 2
        here = (x - 1, pl.ds(y, ROWS), slice(None))
        rows = pl.ds(PY + y, ROWS)
        mid = d[slot, x, rows, mid_z]
        px = d[slot, x + 1, rows, mid_z]
        mx = d[slot, x - 1, rows, mid_z]
        py = d[slot, x, pl.ds(PY + y + 1, ROWS), mid_z]
        my = d[slot, x, pl.ds(PY + y - 1, ROWS), mid_z]
        wide = nz + PZ
        pz = pltpu.roll(d[slot, x, rows, pl.ds(PZ, wide)], wide - 1, 1)[:, :nz]
        mz = pltpu.roll(d[slot, x, rows, pl.ds(0, wide)], 1, 1)[:, PZ:]
        beside = ((px + mx) + (py + my)) + (pz + mz)
        skew = coef[0, *here] * (px - mx) + coef[1, *here] * (py - my)
        skew = skew + coef[2, *here] * (pz - mz)
        applied = (6.0 + coef[3, *here]) * mid - (beside - skew)
        if k == 0:
            left = mid - (1.0 / centre) * applied
            sol[here] = (1.0 / centre) * mid
        else:
            left = res[here] - applied
            sol[here] = sol[here] + mid
        res[here] = left
        if k + 1 < ITERS:
            keep = weights[k + 1] * weights[k] * (1.0 / centre if k == 0 else 1.0)
            d[other, x, rows, mid_z] = keep * mid + (
                2.0 * weights[k + 1] / half_width
            ) * left
            return None
        return left * left

    def add(total, term):
        return total if term is None else total + term

    two = d.at[0, pl.ds(1, 2), mid_y, mid_z]
    pltpu.make_async_copy(two, two, rhs_sem.at[0]).wait()
    for c in order:
        start_x(0, c)
    load_rhs[2].wait()

    def pack_first(x, carry):
        for c in (FIRST, LAST):
            pack(0, x, c)
        return carry

    lax.fori_loop(1, nx + 1, pack_first, 0)
    for c in order:
        open_each(0, c, "start")

    total = jnp.zeros((ROWS, nz), jnp.float32)
    for k in range(ITERS):
        slot, other = k % 2, (k + 1) % 2
        more = k + 1 < ITERS
        for c in order:
            if k == 0:
                if c != LAST:
                    block_of = coef.at[:, :, landed(c)]
                    pltpu.make_async_copy(
                        block_of, block_of, load_sem.at[c // 2]
                    ).wait()
            open_each(slot, c, "wait_recv")
            if k > 0 and c == order[0]:
                sent(other)

            def planes(xs, total, k=k, c=c, slot=slot, other=other, more=more):
                for x in xs:
                    unpack(slot, x, c)
                for x in xs:
                    for y in range(chunks[c][0], sum(chunks[c]), ROWS):
                        total = add(total, block(k, x, y))
                if more:
                    for x in xs:
                        pack(other, x, c)
                return total

            def group(i, total, planes=planes):
                return planes([2 + i * GROUP + j for j in range(GROUP)], total)

            total = lax.fori_loop(0, (nx - 2) // GROUP, group, total)
            for side in (LOW, HIGH):
                x_copy(slot, side, c).wait_recv()
            total = planes((1, nx), total)
            if more:
                start_x(other, c)
                open_each(other, c, "start")

    tile = total[:, :PZ]
    for z in range(PZ, nz, PZ):
        tile = tile + total[:, z : z + PZ]
    tile = jnp.sum(tile, axis=0, keepdims=True)
    first = 0
    for phase, axes in enumerate(phases(sizes)):
        group = phase_steps(sizes, axes)
        own = jnp.int32(0)
        for axis in axes:
            own = own * sizes[axis] + me[axis]
        part[first + own] = tile

        def message(source, steps):
            return pltpu.make_async_remote_copy(
                src_ref=source,
                dst_ref=source,
                send_sem=ps_sem.at[phase],
                recv_sem=pr_sem.at[phase],
                device_id=shifted(steps),
                device_id_type=pl.DeviceIdType.MESH,
            )

        for steps in group:
            message(part.at[first + own], steps).start()
        whole = message(part.at[pl.ds(first, len(group))], group[0])
        if phase == 0:
            sent((ITERS - 1) % 2)
        whole.wait_send()
        whole.wait_recv()
        tile = part[first]
        for p in range(1, len(group) + 1):
            tile = tile + part[first + p]
        first += len(group) + 1
    sums[...] = tile


def put_out(cells, sol, res, sums, sol_out, res_out, norm_out, norm, sem):
    copies = [
        pltpu.make_async_copy(source, target, sem.at[i])
        for i, (source, target) in enumerate(
            ((sol, sol_out), (res, res_out), (norm, norm_out))
        )
    ]
    copies[0].start()
    copies[1].start()
    mean = jnp.sum(sums[...], keepdims=True) / cells
    norm[...] = jnp.broadcast_to(jnp.sqrt(mean + 1e-06), norm.shape)
    copies[2].start()
    for copy in copies:
        copy.wait()


def local(sizes, right_side, reaction, velocity):
    nx, ny, nz = right_side.shape
    hbm = pl.BlockSpec(memory_space=pltpu.HBM)
    vmem = pl.BlockSpec(memory_space=pltpu.VMEM)
    dma = pltpu.SemaphoreType.DMA
    field = jax.ShapeDtypeStruct((nx, ny, nz), jnp.float32)
    sol, res, sums = pl.pallas_call(
        functools.partial(kernel, sizes),
        out_shape=(field, field, jax.ShapeDtypeStruct((1, PZ), jnp.float32)),
        in_specs=[hbm] * 3,
        out_specs=(vmem, vmem, vmem),
        scratch_shapes=[
            pltpu.VMEM((2, nx + 2, ny + 2 * PY, nz + 2 * PZ), jnp.float32),
            pltpu.VMEM((4, nx, ny, nz), jnp.float32),
            pltpu.VMEM((2, 2, nx, 1, nz), jnp.float32),
            pltpu.VMEM((2, 2, nx, 1, nz), jnp.float32),
            pltpu.VMEM((phase_slots(sizes), 1, PZ), jnp.float32),
            dma((2,)),
            dma((2,)),
            dma((2,)),
            dma((2, 2, CHUNKS)),
            dma((2, 2)),
            dma((2, 2)),
            dma((2,)),
            dma((2, 2)),
            dma((len(phases(sizes)),)),
            dma((len(phases(sizes)),)),
        ],
        compiler_params=pltpu.CompilerParams(
            collective_id=0,
            has_side_effects=True,
            vmem_limit_bytes=40 * 1024 * 1024,
        ),
    )(
        *(
            pltpu.with_memory_space_constraint(a, pltpu.HBM)
            for a in (right_side, reaction, velocity)
        )
    )
    cells = nx * ny * nz * sizes[0] * sizes[1] * sizes[2]
    sol, res, norm = pl.pallas_call(
        functools.partial(put_out, cells),
        out_shape=(field, field, jax.ShapeDtypeStruct((1, PZ), jnp.float32)),
        in_specs=[vmem] * 3,
        out_specs=(hbm,) * 3,
        scratch_shapes=[pltpu.VMEM((1, PZ), jnp.float32), dma((3,))],
        compiler_params=pltpu.CompilerParams(vmem_limit_bytes=16 * 1024 * 1024),
    )(sol, res, sums)
    return sol, res, norm[0, 0]


def solution(mesh):
    sizes = tuple(mesh.shape[a] for a in AXES)
    return jax.shard_map(
        functools.partial(local, sizes),
        mesh=mesh,
        in_specs=(P("gx", "gy", "gz"), P("gx", "gy", "gz"), P(None, "gx", "gy", "gz")),
        out_specs=(P("gx", "gy", "gz"), P("gx", "gy", "gz"), P()),
        check_vma=False,
    )
```
